32 devices in a mesh: dp: 8 (over z, x), tensor: 4 (over y, core).
Axes of the slice: x: 2, y: 2, z: 4, core: 2. Of those that a mesh axis runs over, the one named last changes fastest.
Arguments:
- ranges: bfloat16 [10240, 2652], P('dp'), may hold values from 0.049804688 to 2
- pot: float32 [10240], P('dp'), may hold values from 0.1 to 1
- w_ranges: bfloat16 [2652, 2048], P(None, 'tensor'), may hold values from -0.125 to 0.125
- w_pot: float32 [2048], P('tensor'), may hold values from -5 to 5
- bias_one: float32 [2048], P('tensor'), may hold values from -1.5 to 1.5
- w_two: bfloat16 [2048, 2048], P('dp', 'tensor'), may hold values from -0.125 to 0.125
- bias_two: float32 [2048], P('tensor'), may hold values from -1.5 to 1.5
- w_three: bfloat16 [2048, 2048], P('dp', 'tensor'), may hold values from -0.125 to 0.125
- bias_three: float32 [2048], P('tensor'), may hold values from -1.5 to 1.5
- w_out: bfloat16 [2048, 2652], P(('dp', 'tensor')), may hold values from -0.1875 to 0.1875
- bias_out: float32 [2652], replicated, may hold values from -1.5 to 1.5
Outputs:
- hand_values: float32 [10240, 2652], P(('dp', 'tensor'))
The draws below stay inside these ranges and needn't reach their ends.
All inputs are finite; a program needn't handle non-finite values.
Results may differ from the reference program's by a relative error of at most 0.0039.
Values may be sent and summed in bfloat16 or wider, within the bound.
No kernel may reach another device: no remote copies, remote signals or barrier semaphores. Data moves between devices by JAX's collectives and lax.ppermute only.
A program may use at most 128 MiB of HBM per device.

```python
import math
import jax
import jax.numpy as jnp

HANDS = 1326
HID = 2048
STATES = 10240


def spiked(values, own_key, source, target, blocks, factor):
    def block_of(axis_at):
        return (jnp.arange(values.shape[axis_at]) // (values.shape[axis_at] // blocks)).reshape((-1,) + (1,) * (values.ndim - 1 - axis_at))

    near = jax.random.permutation(own_key, blocks)[block_of(target)]
    far = (block_of(target) + blocks // 2) % blocks
    return jnp.where((block_of(source) == near) | (block_of(source) == far), factor * values, values)


def block_scale(stream_key, shape, cuts, least, top_value):
    level = 1.0
    for dim, shards_of in cuts:
        steps = jax.random.uniform(jax.random.fold_in(jax.random.fold_in(stream_key, 6), dim), (shards_of,), jnp.float32, least / len(cuts), top_value / len(cuts))
        level = level * jnp.repeat(jnp.exp(steps), shape[dim] // shards_of).reshape((-1,) + (1,) * (len(shape) - 1 - dim))
    return level


def gaussian(rng, extent, deviation, bound, split=(), held_as=jnp.bfloat16):
    loudness = block_scale(rng, extent, split, -0.22, 0.18) if split else 1.0
    array = jax.random.normal(rng, extent, jnp.float32) * deviation * loudness
    return jnp.minimum(jnp.maximum(array, -bound), bound).astype(held_as)


def heavy_noise(rng, extent, spread, reach, pieces, heavy, dtype=jnp.bfloat16):
    drawn = spread * jax.random.normal(rng, extent, jnp.float32)
    if pieces:
        drawn = drawn * block_scale(rng, extent, pieces, -0.22, 0.18)
    return jnp.clip(spiked(drawn, jax.random.fold_in(rng, 3), *heavy), -reach, reach).astype(dtype)


def setup_inputs(seed: int = 0) -> dict:
    key_list = jax.random.split(jax.random.key(seed), 12)
    return {
        "ranges": jnp.clip(jnp.exp(math.log(2.0) - 3.6927934 * jax.random.uniform(key_list[0], (STATES, 2 * HANDS), jnp.float32) ** block_scale(key_list[0], (STATES, 2 * HANDS), ((0, 8),), -0.2, 0.2)), 0.049804688, 2.0).astype(jnp.bfloat16),
        "pot": jnp.clip(jnp.exp(math.log(1.0) - 2.3025851 * jax.random.uniform(key_list[1], (STATES,), jnp.float32) ** block_scale(key_list[1], (STATES,), ((0, 8),), -0.2, 0.2)), 0.1, 1.0),
        "w_ranges": gaussian(key_list[2], (2 * HANDS, HID), (2 * HANDS) ** -0.5, 0.125, ((1, 4),)),
        "w_pot": gaussian(key_list[3], (HID,), 1.0, 5.0, ((0, 4),), jnp.float32),
        "bias_one": gaussian(key_list[4], (HID,), 0.3, 1.5, ((0, 4),), jnp.float32),
        "w_two": gaussian(key_list[5], (HID, HID), HID ** -0.5, 0.125, ((0, 8), (1, 4))),
        "bias_two": gaussian(key_list[6], (HID,), 0.3, 1.5, ((0, 4),), jnp.float32),
        "w_three": gaussian(key_list[7], (HID, HID), HID ** -0.5, 0.125, ((0, 8), (1, 4))),
        "bias_three": gaussian(key_list[8], (HID,), 0.3, 1.5, ((0, 4),), jnp.float32),
        "w_out": heavy_noise(key_list[9], (HID, 2 * HANDS), HID ** -0.5, 0.1875, ((0, 32),), (0, 1, 4, 2.0)),
        "bias_out": gaussian(key_list[10], (2 * HANDS,), 0.3, 1.5, (), jnp.float32),
    }


def reference(ranges, pot, w_ranges, w_pot, bias_one, w_two, bias_two, w_three, bias_three, w_out, bias_out):
    pre = jnp.dot(ranges, w_ranges, preferred_element_type=jnp.float32)
    pre = pre + pot[:, None] * w_pot[None, :] + bias_one[None, :]
    first = jnp.maximum(pre, 0.0).astype(jnp.bfloat16)
    second = jnp.maximum(jnp.dot(first, w_two, preferred_element_type=jnp.float32) + bias_two[None, :], 0.0).astype(jnp.bfloat16)
    third = jnp.maximum(jnp.dot(second, w_three, preferred_element_type=jnp.float32) + bias_three[None, :], 0.0).astype(jnp.bfloat16)
    values = jnp.dot(third, w_out, preferred_element_type=jnp.float32) + bias_out[None, :]
    weights = ranges.astype(jnp.float32)
    error = jnp.sum(weights * values, axis=1) / jnp.sum(weights, axis=1)
    return values - error[:, None]
```

```python
import jax
import jax.numpy as jnp
from jax import lax
from jax.experimental import pallas as pl
from jax.experimental.pallas import tpu as pltpu
from jax.sharding import PartitionSpec as P

CORES = 2
VMEM_BYTES = 58 * 1024 * 1024


def cycle_of(count):
    slow = count
    for guess in range(1, count + 1):
        if count % guess == 0 and guess * guess >= count:
            slow = guess
            break
    fast = count // slow
    if slow % 2 or fast == 1:
        return list(range(count))
    walk = []
    for row in range(slow):
        columns = range(1, fast) if row % 2 == 0 else range(fast - 1, 0, -1)
        walk += [row * fast + column for column in columns]
    return walk + [row * fast for row in range(slow - 1, -1, -1)]


class Places:
    def __init__(self):
        self.dp = lax.axis_size("dp")
        self.groups = lax.axis_size("tensor")
        self.chips = self.groups // CORES
        self.walk = cycle_of(self.dp)
        position = lax.axis_index("tensor")
        self.chip = position // CORES
        self.core = position % CORES
        rank_of = [self.walk.index(place) for place in range(self.dp)]
        self.rank = jnp.array(rank_of, jnp.int32)[lax.axis_index("dp")]

    def ring(self, array, step):
        count = self.dp
        pairs = [(self.walk[at], self.walk[(at + step) % count]) for at in range(count)]
        return lax.ppermute(array, "dp", pairs)

    def hop(self, array, chips):
        pairs = [
            (place, ((place // CORES + chips) % self.chips) * CORES + place % CORES)
            for place in range(self.groups)
        ]
        return lax.ppermute(array, "tensor", pairs)

    def swap(self, array):
        pairs = [(place, place ^ 1) for place in range(self.groups)]
        return lax.ppermute(array, "tensor", pairs)

    def source(self, back):
        return jnp.array(self.walk, jnp.int32)[(self.rank - back) % self.dp]


def ring_pieces(places, block):
    rows, count = block.shape[0], places.dp
    pieces = [(0, 0, block)]
    forward = backward = block
    for far in range(1, (count - 1) // 2 + 1):
        forward = places.ring(forward, 1)
        backward = places.ring(backward, -1)
        pieces += [(far, 0, forward), (-far, 0, backward)]
    if count > 1 and count % 2 == 0:
        half = rows // 2
        pieces += [
            (count // 2, 0, places.ring(forward[:half], 1)),
            (count // 2, half, places.ring(backward[half:], -1)),
        ]
    return pieces


def over_chips(places, array):
    out = [array]
    for _ in range(1, places.chips):
        out.append(places.hop(out[-1], 1))
    return out


def gather_late(places, block):
    return [(back, row, over_chips(places, piece)) for back, row, piece in ring_pieces(places, block)]


def gather_early(places, block):
    wide = jnp.concatenate(over_chips(places, block), axis=1)
    return [(back, row, [piece]) for back, row, piece in ring_pieces(places, wide)]


def hidden_layer(places, own, peer, pieces, bias, units, split):
    chips, rows, width = own.shape
    per = width // units
    flat, layout = [], []
    for back, row, parts in pieces:
        layout.append((row, parts[0].shape[0], len(parts)))
        flat += parts
    scalars = jnp.stack(
        [places.chip, places.core] + [places.source(back) for back, _, _ in pieces]
    ).astype(jnp.int32)
    halves = CORES if split else 1
    part_rows = rows // halves

    def kernel(at, own_ref, peer_ref, bias_ref, *rest):
        weights = rest[: len(flat)]
        outs = rest[len(flat) : len(flat) + halves]
        hidden = rest[-1]
        for back in range(chips):
            chip = lax.rem(at[0] - back + chips, chips)
            for ref, core in ((own_ref, at[1]), (peer_ref, 1 - at[1])):
                for piece in range(per):
                    hidden[(chip * CORES + core) * per + piece] = ref[
                        back, :, piece * units : (piece + 1) * units
                    ]
        for half in range(halves):
            start = 0 if half == 0 else part_rows
            if split:
                start = pl.multiple_of(part_rows * (at[1] if half == 0 else 1 - at[1]), part_rows)
            for back in range(chips):
                total = None
                first = 0
                for number, (row, height, parts) in enumerate(layout):
                    left = hidden[at[2 + number], pl.ds(start, part_rows), row : row + height]
                    if parts == 1:
                        right = weights[first][:, back * width : (back + 1) * width]
                    else:
                        right = weights[first + back][...]
                    first += parts
                    term = jnp.dot(left, right, preferred_element_type=jnp.float32)
                    total = term if total is None else total + term
                total = total + bias_ref[back : back + 1, :]
                outs[half][back] = jnp.maximum(total, 0.0).astype(jnp.bfloat16)

    whole = pl.BlockSpec(memory_space=pltpu.VMEM)
    shape = jax.ShapeDtypeStruct((chips, part_rows, width), jnp.bfloat16)
    return pl.pallas_call(
        kernel,
        out_shape=[shape] * halves,
        in_specs=[pl.BlockSpec(memory_space=pltpu.SMEM)] + [whole] * (3 + len(flat)),
        out_specs=[whole] * halves,
        scratch_shapes=[pltpu.VMEM((chips * CORES * per, rows, units), jnp.bfloat16)],
        compiler_params=pltpu.CompilerParams(vmem_limit_bytes=VMEM_BYTES),
    )(scalars, own, peer, bias, *flat)


def output_layer(places, own, peer, pieces, bias, ranges):
    chips, rows, width = own.shape
    units = width * chips * CORES // places.dp
    per = width // units
    share = units // CORES
    columns = ranges.shape[1]
    flat, layout = [], []
    for back, row, mine, other in pieces:
        layout.append((row, mine.shape[0]))
        flat += [mine, other]
    scalars = jnp.stack(
        [places.chip, places.core] + [places.source(piece[0]) for piece in pieces]
    ).astype(jnp.int32)
    tile = 512

    def kernel(at, own_ref, peer_ref, bias_ref, ranges_ref, *rest):
        weights = rest[: len(flat)]
        out = rest[len(flat)]
        hidden = rest[-1]
        for back in range(chips):
            chip = lax.rem(at[0] - back + chips, chips)
            for ref, core in ((own_ref, at[1]), (peer_ref, 1 - at[1])):
                for piece in range(per):
                    for side in range(CORES):
                        first = piece * units + side * share
                        hidden[(chip * CORES + core) * per + piece, side] = ref[
                            back, :, first : first + share
                        ]
        upper = jnp.zeros((rows, 1), jnp.float32)
        lower = jnp.zeros((rows, 1), jnp.float32)
        for first in range(0, columns, tile):
            last = min(first + tile, columns)
            total = None
            for number, (row, height) in enumerate(layout):
                place = at[2 + number]
                left = jnp.concatenate(
                    [
                        hidden[place, at[1], :, row : row + height],
                        hidden[place, 1 - at[1], :, row : row + height],
                    ],
                    axis=1,
                )
                right = jnp.concatenate(
                    [weights[2 * number][:, first:last], weights[2 * number + 1][:, first:last]], axis=0
                )
                term = jnp.dot(left, right, preferred_element_type=jnp.float32)
                total = term if total is None else total + term
            total = total + bias_ref[:, first:last]
            out[:, first:last] = total
            amount = ranges_ref[:, first:last].astype(jnp.float32)
            upper = upper + jnp.sum(amount * total, axis=1, keepdims=True)
            lower = lower + jnp.sum(amount, axis=1, keepdims=True)
        out[...] = out[...] - upper / lower

    whole = pl.BlockSpec(memory_space=pltpu.VMEM)
    return pl.pallas_call(
        kernel,
        out_shape=jax.ShapeDtypeStruct((rows, columns), jnp.float32),
        in_specs=[pl.BlockSpec(memory_space=pltpu.SMEM)] + [whole] * (4 + len(flat)),
        out_specs=whole,
        scratch_shapes=[pltpu.VMEM((places.dp, CORES, rows, share), jnp.bfloat16)],
        compiler_params=pltpu.CompilerParams(vmem_limit_bytes=VMEM_BYTES),
    )(scalars, own, peer, bias[None, :], ranges, *flat)


def local(
    ranges, pot, w_ranges, w_pot, bias_one, w_two, bias_two, w_three, bias_three, w_out, bias_out
):
    places = Places()
    chips, groups = places.chips, places.groups
    states, width = ranges.shape[0], w_pot.shape[0]
    units = width * groups // places.dp
    small = w_out.shape[0]

    def by_core(array):
        lead = array.shape[:-1]
        blocks = array.reshape(lead + (width // units, chips, CORES, small))
        return jnp.swapaxes(blocks, -3, -2).reshape(lead + (width,))

    w_three, bias_three = by_core(w_three), by_core(bias_three)

    two = gather_late(places, w_two)
    cut = w_three.shape[0] // 2
    third_late = gather_late(places, w_three[:cut])
    third_early = gather_early(places, w_three[cut:])
    three = third_late + [(back, row + cut, parts) for back, row, parts in third_early]

    stack = jnp.zeros((chips,) + w_out.shape, w_out.dtype)
    for back, part in enumerate(over_chips(places, w_out)):
        stack = lax.dynamic_update_index_in_dim(stack, part, (places.chip - back) % chips, 0)
    ring = ring_pieces(places, stack.reshape(chips * small, -1))
    out_pieces = [(back, row, piece, places.swap(piece)) for back, row, piece in ring]

    biases = over_chips(places, jnp.stack([bias_two, bias_three]))
    bias_two = jnp.stack([pair[0] for pair in biases])
    bias_three = jnp.stack([pair[1] for pair in biases])

    pre = jnp.dot(ranges, w_ranges, preferred_element_type=jnp.float32)
    pre = pre + pot[:, None] * w_pot[None, :] + bias_one[None, :]
    first = jnp.maximum(pre, 0.0).astype(jnp.bfloat16)

    rows = states // chips
    blocks = []
    for back in range(chips):
        part = lax.dynamic_slice_in_dim(first, ((places.chip + back) % chips) * rows, rows, 0)
        blocks.append(places.hop(part, back) if back else part)
    own = jnp.stack(blocks)
    (own,) = hidden_layer(places, own, places.swap(own), two, bias_two, units, False)
    keep, send = hidden_layer(places, own, places.swap(own), three, bias_three, units, True)

    count = states // groups
    own_ranges = lax.dynamic_slice_in_dim(ranges, lax.axis_index("tensor") * count, count, 0)
    return output_layer(places, keep, places.swap(send), out_pieces, bias_out, own_ranges)


def solution(mesh):
    in_specs = (
        P("dp", None),
        P("dp"),
        P(None, "tensor"),
        P("tensor"),
        P("tensor"),
        P("dp", "tensor"),
        P("tensor"),
        P("dp", "tensor"),
        P("tensor"),
        P(("dp", "tensor"), None),
        P(),
    )
    out_specs = P(("dp", "tensor"), None)
    return jax.shard_map(local, mesh=mesh, in_specs=in_specs, out_specs=out_specs, check_vma=False)
```

```python
import jax
import jax.numpy as jnp
from jax import lax
from jax.experimental import pallas as pl
from jax.experimental.pallas import tpu as pltpu
from jax.sharding import PartitionSpec as P

CORES = 2
VMEM_BYTES = 58 * 1024 * 1024


def cycle_of(count):
    slow = count
    for guess in range(1, count + 1):
        if count % guess == 0 and guess * guess >= count:
            slow = guess
            break
    fast = count // slow
    if slow % 2 or fast == 1:
        return list(range(count))
    walk = []
    for row in range(slow):
        columns = range(1, fast) if row % 2 == 0 else range(fast - 1, 0, -1)
        walk += [row * fast + column for column in columns]
    return walk + [row * fast for row in range(slow - 1, -1, -1)]


class Places:
    def __init__(self):
        self.dp = lax.axis_size("dp")
        self.groups = lax.axis_size("tensor")
        self.chips = self.groups // CORES
        self.walk = cycle_of(self.dp)
        position = lax.axis_index("tensor")
        self.chip = position // CORES
        self.core = position % CORES

    def ring(self, array, step):
        count = self.dp
        pairs = [(self.walk[at], self.walk[(at + step) % count]) for at in range(count)]
        return lax.ppermute(array, "dp", pairs)

    def hop(self, array, chips):
        pairs = [
            (place, ((place // CORES + chips) % self.chips) * CORES + place % CORES)
            for place in range(self.groups)
        ]
        return lax.ppermute(array, "tensor", pairs)

    def swap(self, array):
        pairs = [(place, place ^ 1) for place in range(self.groups)]
        return lax.ppermute(array, "tensor", pairs)

    def scalars(self, backs):
        at = [self.walk.index(place) for place in range(self.dp)]
        table = [[self.walk[(rank - back) % self.dp] for back in backs] for rank in at]
        here = jnp.stack([self.chip, self.core]).astype(jnp.int32)
        if not backs:
            return here
        row = lax.dynamic_index_in_dim(
            jnp.array(table, jnp.int32), lax.axis_index("dp"), 0, keepdims=False
        )
        return jnp.concatenate([here, row])


def ring_pieces(places, block):
    rows, count = block.shape[0], places.dp
    pieces = [(0, 0, block)]
    forward = backward = block
    for far in range(1, (count - 1) // 2 + 1):
        forward = places.ring(forward, 1)
        backward = places.ring(backward, -1)
        pieces += [(far, 0, forward), (-far, 0, backward)]
    if count > 1 and count % 2 == 0:
        half = rows // 2
        pieces += [
            (count // 2, 0, places.ring(forward[:half], 1)),
            (count // 2, half, places.ring(backward[half:], -1)),
        ]
    return pieces


def over_chips(places, array):
    out = [array]
    for _ in range(1, places.chips):
        out.append(places.hop(out[-1], 1))
    return out


def hidden_layer(places, own, peer, pieces, bias, units, split):
    chips, rows, width = own.shape
    per = width // units
    flat, layout, backs = [], [], []
    for back, row, parts in pieces:
        if back is None:
            for place in range(places.dp):
                layout.append((place, None, row, units, len(flat), place * units))
        else:
            layout.append((None, 2 + len(backs), row, parts[0].shape[0], len(flat), 0))
            backs.append(back)
        flat += parts
    scalars = places.scalars(backs)
    halves = CORES if split else 1
    part_rows = rows // halves

    def kernel(at, own_ref, peer_ref, bias_ref, *rest):
        weights = rest[: len(flat)]
        outs = rest[len(flat) : len(flat) + halves]
        hidden = rest[-1]
        for back in range(chips):
            chip = lax.rem(at[0] - back + chips, chips)
            for ref, core in ((own_ref, at[1]), (peer_ref, 1 - at[1])):
                for piece in range(per):
                    hidden[(chip * CORES + core) * per + piece] = ref[
                        back, :, piece * units : (piece + 1) * units
                    ]
        for half in range(halves):
            start = 0 if half == 0 else part_rows
            if split:
                start = pl.multiple_of(part_rows * (at[1] if half == 0 else 1 - at[1]), part_rows)
            for back in range(chips):
                total = None
                for place, scalar, row, height, first, top in layout:
                    place = at[scalar] if place is None else place
                    left = hidden[place, pl.ds(start, part_rows), row : row + height]
                    right = weights[first + back][top : top + height, :]
                    term = jnp.dot(left, right, preferred_element_type=jnp.float32)
                    total = term if total is None else total + term
                total = total + bias_ref[back : back + 1, :]
                outs[half][back] = jnp.maximum(total, 0.0).astype(jnp.bfloat16)

    whole = pl.BlockSpec(memory_space=pltpu.VMEM)
    shape = jax.ShapeDtypeStruct((chips, part_rows, width), jnp.bfloat16)
    return pl.pallas_call(
        kernel,
        out_shape=[shape] * halves,
        in_specs=[pl.BlockSpec(memory_space=pltpu.SMEM)] + [whole] * (3 + len(flat)),
        out_specs=[whole] * halves,
        scratch_shapes=[pltpu.VMEM((chips * CORES * per, rows, units), jnp.bfloat16)],
        compiler_params=pltpu.CompilerParams(vmem_limit_bytes=VMEM_BYTES),
    )(scalars, own, peer, bias, *flat)


def output_layer(places, own, peer, mine, other, bias, ranges):
    chips, rows, width = own.shape
    units = width * chips * CORES // places.dp
    per = width // units
    share = units // CORES
    columns = bias.shape[0]
    scalars = places.scalars([])
    tile = 512

    def kernel(at, own_ref, peer_ref, bias_ref, ranges_ref, mine_ref, other_ref, out, hidden):
        for back in range(chips):
            chip = lax.rem(at[0] - back + chips, chips)
            for ref, core in ((own_ref, at[1]), (peer_ref, 1 - at[1])):
                for piece in range(per):
                    for side in range(CORES):
                        first = piece * units + side * share
                        hidden[(chip * CORES + core) * per + piece, side] = ref[
                            back, :, first : first + share
                        ]
        upper = jnp.zeros((rows, 1), jnp.float32)
        lower = jnp.zeros((rows, 1), jnp.float32)
        for first in range(0, columns, tile):
            last = min(first + tile, columns)
            total = None
            for place in range(places.dp):
                left = jnp.concatenate(
                    [hidden[place, at[1]], hidden[place, 1 - at[1]]], axis=1
                )
                rows_of = slice(place * share, (place + 1) * share)
                right = jnp.concatenate(
                    [mine_ref[rows_of, first:last], other_ref[rows_of, first:last]], axis=0
                )
                term = jnp.dot(left, right, preferred_element_type=jnp.float32)
                total = term if total is None else total + term
            total = total + bias_ref[:, first:last]
            out[:, first:last] = total
            amount = ranges_ref[:, first:last].astype(jnp.float32)
            upper = upper + jnp.sum(amount * total, axis=1, keepdims=True)
            lower = lower + jnp.sum(amount, axis=1, keepdims=True)
        out[...] = out[...] - upper / lower

    whole = pl.BlockSpec(memory_space=pltpu.VMEM)
    return pl.pallas_call(
        kernel,
        out_shape=jax.ShapeDtypeStruct((rows, columns), jnp.float32),
        in_specs=[pl.BlockSpec(memory_space=pltpu.SMEM)] + [whole] * 6,
        out_specs=whole,
        scratch_shapes=[pltpu.VMEM((places.dp, CORES, rows, share), jnp.bfloat16)],
        compiler_params=pltpu.CompilerParams(vmem_limit_bytes=VMEM_BYTES),
    )(scalars, own, peer, bias[None, :], ranges, mine, other)


def local(
    ranges, pot, w_ranges, w_pot, bias_one, w_two, bias_two, w_three, bias_three, w_out, bias_out
):
    places = Places()
    chips, groups = places.chips, places.groups
    states, width = ranges.shape[0], w_pot.shape[0]
    units = width * groups // places.dp
    small = w_out.shape[0]

    def by_core(array):
        lead = array.shape[:-1]
        blocks = array.reshape(lead + (width // units, chips, CORES, small))
        return jnp.swapaxes(blocks, -3, -2).reshape(lead + (width,))

    w_three, bias_three = by_core(w_three), by_core(bias_three)

    two = ring_pieces(places, w_two)
    third = lax.all_gather(w_three, "dp", axis=0, tiled=True)

    biases = over_chips(places, jnp.stack([bias_two, bias_three]))
    bias_two = jnp.stack([pair[0] for pair in biases])
    bias_three = jnp.stack([pair[1] for pair in biases])

    pre = jnp.dot(ranges, w_ranges, preferred_element_type=jnp.float32)
    pre = pre + pot[:, None] * w_pot[None, :] + bias_one[None, :]
    first = jnp.maximum(pre, 0.0).astype(jnp.bfloat16)

    wide = jnp.pad(w_out, ((0, 0), (0, -w_out.shape[1] % 128)))
    stack = jnp.zeros((chips,) + wide.shape, w_out.dtype)
    for back, part in enumerate(over_chips(places, wide)):
        stack = lax.dynamic_update_index_in_dim(stack, part, (places.chip - back) % chips, 0)
    count = states // groups
    own_ranges = lax.dynamic_slice_in_dim(ranges, lax.axis_index("tensor") * count, count, 0)
    own_ranges = jnp.pad(own_ranges, ((0, 0), (0, -w_out.shape[1] % 128)))
    rows = states // chips
    blocks = []
    for back in range(chips):
        part = lax.dynamic_slice_in_dim(first, ((places.chip + back) % chips) * rows, rows, 0)
        blocks.append(places.hop(part, back) if back else part)
    own = jnp.stack(blocks)

    early = [over_chips(places, piece) for _, _, piece in two[:-2]]
    late = [piece for _, _, piece in two[-2:]]
    stack, third, own_ranges, own, early, late = lax.optimization_barrier(
        (stack, third, own_ranges, own, early, late)
    )
    mine = lax.all_gather(stack.reshape(chips * small, -1), "dp", axis=0, tiled=True)
    thirds = over_chips(places, third)
    late = [over_chips(places, piece) for piece in late]
    own, thirds, late = lax.optimization_barrier((own, thirds, late))
    two = [(back, row, parts) for (back, row, _), parts in zip(two, early + late)]
    three = [(None, 0, thirds)]
    (own,) = hidden_layer(places, own, places.swap(own), two, bias_two, units, False)
    keep, send = hidden_layer(places, own, places.swap(own), three, bias_three, units, True)
    keep, mine = lax.optimization_barrier((keep, mine))
    other = places.swap(mine)

    return output_layer(places, keep, places.swap(send), mine, other, bias_out, own_ranges)


def solution(mesh):
    in_specs = (
        P("dp", None),
        P("dp"),
        P(None, "tensor"),
        P("tensor"),
        P("tensor"),
        P("dp", "tensor"),
        P("tensor"),
        P("dp", "tensor"),
        P("tensor"),
        P(("dp", "tensor"), None),
        P(),
    )
    out_specs = P(("dp", "tensor"), None)
    return jax.shard_map(local, mesh=mesh, in_specs=in_specs, out_specs=out_specs, check_vma=False)
```
